768 devices in a mesh: fsdp: 64 (over x, y, core), blk: 12 (over z).
Axes of the slice: x: 4, y: 8, z: 12, core: 2. Of those that a mesh axis runs over, the one named last changes fastest.
Arguments:
- grad: bfloat16 [128, 768, 768], P(None, 'fsdp', 'blk'), may hold values from -16 to 16
- owner_slots: int32 [128], replicated, may hold values from 0 to 127, as said below
- stat_left: float32 [128, 768, 768], P('fsdp', None, 'blk'), may hold values from -6 to 6
- stat_right: float32 [128, 768, 768], P('fsdp', None, 'blk'), may hold values from -6 to 6
- basis_left: bfloat16 [128, 768, 768], P('fsdp'), may hold values from -1 to 1, as said below
- basis_right: bfloat16 [128, 768, 768], P('fsdp'), may hold values from -1 to 1, as said below
- moment: float32 [128, 768, 768], P('fsdp', None, 'blk'), may hold values from -3 to 3
- second: float32 [128, 768, 768], P('fsdp', None, 'blk'), may hold values from 0.01 to 0.1
Outputs:
- update: bfloat16 [128, 768, 768], P(None, 'fsdp', 'blk')
- new_left: float32 [128, 768, 768], P('fsdp', None, 'blk')
- new_right: float32 [128, 768, 768], P('fsdp', None, 'blk')
- new_moment: float32 [128, 768, 768], P('fsdp', None, 'blk')
- new_second: float32 [128, 768, 768], P('fsdp', None, 'blk')
- grad_rms: float32 [], replicated
The draws below stay inside these ranges and needn't reach their ends.
Inputs may be any that keep to these rules, and one draw needn't show every extreme that they name: Each 768 x 768 block of basis_left is orthogonal up to bfloat16 rounding. Each 768 x 768 block of basis_right is orthogonal up to bfloat16 rounding. owner_slots names every block exactly once.
All inputs are finite; a program needn't handle non-finite values.
Results may differ from the reference program's by a relative error of at most 0.0058.
Values may be sent and summed in bfloat16 or wider, within the bound.
A program may use at most 64 MiB of HBM per device.

```python
import math
import jax
import jax.numpy as jnp
from jax import lax

BS = 768
NBG = 128


def slot_order(key):
    return jax.random.permutation(jax.random.fold_in(key, 77), NBG).astype(jnp.int32)


def draw_owner_slots(key, part):
    return slot_order(key)


def draw_grad(key, part):
    slots = slot_order(key)
    places = jnp.zeros((NBG,), jnp.int32).at[slots].set(jnp.arange(NBG, dtype=jnp.int32))
    level = places.astype(jnp.float32) / (NBG - 1)
    inner = jax.random.fold_in(key, 5)
    rows = jnp.arange(BS, dtype=jnp.float32)
    row_scale = jnp.sqrt(1.0 + 2.0 * rows / (BS - 1))
    scale = row_scale[None, :, None] * row_scale[None, None, :]
    block_scale = jnp.sqrt(1.0 + 8.0 * level)
    values = 0.5 * jax.random.normal(inner, (NBG, BS, BS), jnp.float32) * scale * block_scale[:, None, None]
    return jnp.clip(values, -16.0, 16.0).astype(jnp.bfloat16)


def orthogonal(key):
    matrix = jax.random.normal(key, (NBG, BS, BS), jnp.float32)
    basis, upper = jnp.linalg.qr(matrix)
    return basis.astype(jnp.bfloat16)


def draw_basis_left(key, part):
    return orthogonal(jax.random.fold_in(key, 11))


def draw_basis_right(key, part):
    return orthogonal(jax.random.fold_in(key, 23))


def block_levels(own_key, shape, split, low, top_value):
    level = 1.0
    for position, parts in split:
        draws = jax.random.uniform(jax.random.fold_in(jax.random.fold_in(own_key, 6), position), (parts,), jnp.float32, low / len(split), top_value / len(split))
        level = level * jnp.repeat(jnp.exp(draws), shape[position] // parts).reshape((-1,) + (1,) * (len(shape) - 1 - position))
    return level


def centred(stream_key, dims, scale, reach, cuts=(), kind=jnp.bfloat16):
    drawn = jax.random.normal(stream_key, dims, jnp.float32) * scale
    if len(cuts) > 0:
        drawn = block_levels(stream_key, dims, cuts, -0.22, 0.18) * drawn
    return jnp.clip(drawn, min=-reach, max=reach).astype(kind)


def setup_inputs(seed: int = 0) -> dict:
    seeds = jax.random.split(jax.random.key(seed), 9)
    return {
        "grad": draw_grad(jax.random.fold_in(seeds[8], 71), 0),
        "owner_slots": draw_owner_slots(jax.random.fold_in(seeds[8], 71), 0),
        "stat_left": centred(seeds[2], (NBG, BS, BS), 1.0, 6.0, ((0, 64), (2, 12)), jnp.float32),
        "stat_right": centred(seeds[3], (NBG, BS, BS), 1.0, 6.0, ((0, 64), (2, 12)), jnp.float32),
        "basis_left": draw_basis_left(jax.random.fold_in(seeds[8], 71), 0),
        "basis_right": draw_basis_right(jax.random.fold_in(seeds[8], 71), 0),
        "moment": centred(seeds[6], (NBG, BS, BS), 0.2, 3.0, ((0, 64), (2, 12)), jnp.float32),
        "second": jnp.clip(jnp.exp(math.log(0.1) - 2.3025851 * jax.random.uniform(seeds[7], (NBG, BS, BS), jnp.float32) ** block_levels(seeds[7], (NBG, BS, BS), ((0, 64), (2, 12)), -0.2, 0.2)), 0.01, 0.1),
    }


clip_level = 0.5
stat_decay = 0.95
beta_one = 0.9
beta_two = 0.95
epsilon = 1e-08

def reference(grad, owner_slots, stat_left, stat_right, basis_left, basis_right, moment, second):
    total = jnp.sum(jnp.square(grad.astype(jnp.float32)))
    grad_rms = jnp.sqrt(total / (NBG * BS * BS))
    factor = jnp.minimum(1.0, clip_level / grad_rms)

    def one_block(index):
        which = owner_slots[index]
        block = grad[which]
        q_left = basis_left[index]
        q_right = basis_right[index]
        outer_left = jnp.dot(block.astype(jnp.float32), block.T.astype(jnp.float32), preferred_element_type=jnp.float32)
        outer_right = jnp.dot(block.T.astype(jnp.float32), block.astype(jnp.float32), preferred_element_type=jnp.float32)
        new_l = stat_decay * stat_left[index] + (1.0 - stat_decay) * (factor * factor) * outer_left
        new_r = stat_decay * stat_right[index] + (1.0 - stat_decay) * (factor * factor) * outer_right
        turned = jnp.dot(block.astype(jnp.float32), q_right.astype(jnp.float32), preferred_element_type=jnp.float32).astype(jnp.bfloat16)
        rotated = factor * jnp.dot(q_left.T.astype(jnp.float32), turned.astype(jnp.float32), preferred_element_type=jnp.float32)
        new_m = beta_one * moment[index] + (1.0 - beta_one) * rotated
        new_v = beta_two * second[index] + (1.0 - beta_two) * rotated * rotated
        scaled = (new_m / (jnp.sqrt(new_v) + epsilon)).astype(jnp.bfloat16)
        back = jnp.dot(q_left.astype(jnp.float32), scaled.astype(jnp.float32), preferred_element_type=jnp.float32).astype(jnp.bfloat16)
        step = jnp.dot(back.astype(jnp.float32), q_right.T.astype(jnp.float32), preferred_element_type=jnp.float32).astype(jnp.bfloat16)
        return (step, new_l, new_r, new_m, new_v)
    steps, new_left, new_right, new_moment, new_second = lax.map(one_block, jnp.arange(NBG, dtype=jnp.int32))
    update = jnp.zeros_like(steps).at[owner_slots].set(steps)
    return (update, new_left, new_right, new_moment, new_second, grad_rms)
```

```python
import functools

import jax
import jax.numpy as jnp
from jax import lax
from jax.experimental import pallas as pl
from jax.experimental.pallas import tpu as pltpu
from jax.sharding import PartitionSpec as P

BS = 768
NF = 64
NZ = 12
ROWS = BS // NF
PAD = 16
COLS = BS // NZ
LANES = 128
PER = BS // LANES
SLOTS = 2
PIECES = 2
PIECE = COLS // PIECES

clip_level = 0.5
stat_decay = 0.95
beta_one = 0.9
beta_two = 0.95
epsilon = 1e-08

F32 = jnp.float32
BF16 = jnp.bfloat16


def nn(a, b):
    return lax.dot_general(a, b, (((1,), (0,)), ((), ())), preferred_element_type=F32)


def nt(a, b):
    return lax.dot_general(a, b, (((1,), (1,)), ((), ())), preferred_element_type=F32)


def tn(a, b):
    return lax.dot_general(a, b, (((0,), (0,)), ((), ())), preferred_element_type=F32)


def kernel(
    entries,
    a_hbm,
    ql_hbm,
    qr_hbm,
    left_hbm,
    right_hbm,
    moment_hbm,
    second_hbm,
    w_out,
    left_out,
    right_out,
    moment_out,
    second_out,
    rms_out,
    a_ref,
    x_ref,
    gt_ref,
    ql_ref,
    qr_ref,
    state_ref,
    spread_ref,
    pick_ref,
    cols_ref,
    part_ref,
    plane_parts,
    plane_ref,
    all_parts,
    bt_ref,
    b_ref,
    ut_ref,
    ur_ref,
    u2_ref,
    y_ref,
    w_ref,
    load_sem,
    store_sem,
    x_send,
    x_recv,
    ring_send,
    ring_recv,
    part_send,
    part_recv,
    all_send,
    all_recv,
    b_send,
    b_recv,
    u_send,
    u_recv,
    w_send,
    w_recv,
):
    f = lax.axis_index("fsdp")
    z = lax.axis_index("blk")

    def along_f(step):
        return lax.rem(f + step, NF)

    def along_z(step):
        return lax.rem(z + step, NZ)

    x_ref[...] = jnp.zeros_like(x_ref)

    barrier = pltpu.get_barrier_semaphore()

    def greet_f(step, _):
        pl.semaphore_signal(barrier, inc=1, device_id={"fsdp": along_f(step)}, device_id_type=pl.DeviceIdType.MESH)
        return 0

    def greet_z(step, _):
        pl.semaphore_signal(barrier, inc=1, device_id={"blk": along_z(step)}, device_id_type=pl.DeviceIdType.MESH)
        return 0

    lax.fori_loop(1, NF, greet_f, 0)
    lax.fori_loop(1, NZ, greet_z, 0)

    loads = [
        pltpu.make_async_copy(qr_hbm, qr_ref, load_sem.at[0]),
        pltpu.make_async_copy(ql_hbm, ql_ref, load_sem.at[1]),
        pltpu.make_async_copy(moment_hbm, state_ref.at[0], load_sem.at[2]),
        pltpu.make_async_copy(second_hbm, state_ref.at[1], load_sem.at[3]),
        pltpu.make_async_copy(left_hbm, state_ref.at[2], load_sem.at[4]),
        pltpu.make_async_copy(right_hbm, state_ref.at[3], load_sem.at[5]),
        pltpu.make_async_copy(a_hbm, a_ref, load_sem.at[6]),
    ]
    for load in loads[::-1]:
        load.start()

    q = lax.broadcasted_iota(jnp.int32, spread_ref.shape, 0)
    r = lax.broadcasted_iota(jnp.int32, spread_ref.shape, 1)
    group = q // PAD
    inside = q - group * PAD
    spread_ref[...] = jnp.where((inside < ROWS) & (r == group * ROWS + inside), 1.0, 0.0).astype(BF16)
    k = lax.broadcasted_iota(jnp.int32, pick_ref.shape, 0)
    r = lax.broadcasted_iota(jnp.int32, pick_ref.shape, 1)
    pick_ref[...] = jnp.where(r == z * COLS + k, 1.0, 0.0).astype(BF16)

    loads[6].wait()
    pl.semaphore_wait(barrier, NF - 1 + NZ - 1)

    def exchange_f(src, dst, send, recv, step, src_at=None):
        to = along_f(step)
        return pltpu.make_async_remote_copy(
            src_ref=src if src_at is None else src.at[to, pl.ds(0, ROWS)],
            dst_ref=dst.at[f] if src_at is None else dst.at[f, pl.ds(0, ROWS)],
            send_sem=send.at[0],
            recv_sem=recv.at[0],
            device_id={"fsdp": to},
            device_id_type=pl.DeviceIdType.MESH,
        )

    def exchange_z(src, dst, send, recv, step, src_at=None):
        to = along_z(step)
        return pltpu.make_async_remote_copy(
            src_ref=src if src_at is None else src.at[to],
            dst_ref=dst.at[z],
            send_sem=send.at[0],
            recv_sem=recv.at[0],
            device_id={"blk": to},
            device_id_type=pl.DeviceIdType.MESH,
        )

    def send_all(exchange, count, *refs, **kw):
        def one(step, _):
            exchange(*refs, step, **kw).start()
            return 0

        lax.fori_loop(1, count, one, 0)

    def all_of(ref, count, send, recv, axis, rows=None):
        some = ref.at[pl.ds(0, count - 1)] if rows is None else ref.at[pl.ds(0, count - 1), pl.ds(0, rows)]
        return pltpu.make_async_remote_copy(
            src_ref=some,
            dst_ref=some,
            send_sem=send.at[0],
            recv_sem=recv.at[0],
            device_id={axis: along_f(1) if axis == "fsdp" else along_z(1)},
            device_id_type=pl.DeviceIdType.MESH,
        )

    send_all(exchange_f, NF, a_ref, x_ref, x_send, x_recv, src_at=True)
    x_ref[f, pl.ds(0, ROWS)] = a_ref[f]
    x_all = all_of(x_ref, NF, x_send, x_recv, "fsdp", ROWS)

    loads[0].wait()
    for s in range(SLOTS):
        cols_ref[s] = nt(pick_ref[...], qr_ref[s]).astype(BF16)

    x_all.wait_recv()
    half = NF // 2 * PAD
    wide = BS // 2
    for g in range(2):
        block = x_ref[pl.ds(g * (NF // 2), NF // 2)].reshape(half, LANES)
        panel = tn(block, spread_ref[...]).astype(BF16)
        for s in range(SLOTS):
            gt_ref[s, z, :, pl.ds(g * wide, wide)] = panel[s * COLS : (s + 1) * COLS]
    values = x_ref[...].astype(F32)
    part_ref[...] = jnp.full(part_ref.shape, jnp.sum(values * values), F32)

    hops = {}
    streams = [(s, way, p) for p in range(PIECES) for s in range(SLOTS) for way in range(2)]
    for s, way, p in streams:
        last = NZ // 2 if s == way else NZ // 2 - 1
        for t in range(last):
            origin = along_z(NZ - t) if way == 0 else along_z(t)
            to = along_z(1) if way == 0 else along_z(NZ - 1)
            hops[s, way, p, t] = pltpu.make_async_remote_copy(
                src_ref=gt_ref.at[s, origin, pl.ds(p * PIECE, PIECE)],
                dst_ref=gt_ref.at[s, origin, pl.ds(p * PIECE, PIECE)],
                send_sem=ring_send.at[s, way, p, t],
                recv_sem=ring_recv.at[s, way, p, t],
                device_id={"blk": to},
                device_id_type=pl.DeviceIdType.MESH,
            )

    for t in range(NZ // 2):
        for s, way, p in streams:
            if (s, way, p, t - 1) in hops:
                hops[s, way, p, t - 1].wait_recv()
            if (s, way, p, t) in hops:
                hops[s, way, p, t].start()
        if t == 0:
            send_all(exchange_f, NF, part_ref, plane_parts, part_send, part_recv)
            plane_parts[f] = part_ref[...]
        if t == 2:
            plane_all = all_of(plane_parts, NF, part_send, part_recv, "fsdp")
            plane_all.wait_recv()
            plane_ref[...] = jnp.sum(plane_parts[...], axis=0)
            send_all(exchange_z, NZ, plane_ref, all_parts, all_send, all_recv)
            all_parts[z] = plane_ref[...]
        if t == 4:
            all_all = all_of(all_parts, NZ, all_send, all_recv, "blk")
            all_all.wait_recv()
            total = jnp.sum(all_parts[...], axis=0)
            grad_rms = jnp.sqrt(total / entries)
            rms_out[...] = grad_rms
            part = jnp.minimum(1.0, clip_level / grad_rms)
            factor = jnp.broadcast_to(part[0:1, 0:1], (COLS, BS))
    for load in loads[1:6]:
        load.wait()
    for s, way, p in streams:
        if s == way:
            hops[s, way, p, NZ // 2 - 1].wait_recv()

    stores = []
    for s in range(SLOTS):
        gt = gt_ref[s].reshape(BS, BS)
        turned = nn(cols_ref[s], gt).astype(BF16)
        rotated = factor * nn(turned, ql_ref[s])
        new_moment = beta_one * state_ref[0, s] + (1.0 - beta_one) * rotated
        new_second = beta_two * state_ref[1, s] + (1.0 - beta_two) * rotated * rotated
        state_ref[0, s] = new_moment
        state_ref[1, s] = new_second
        scaled = (new_moment / (jnp.sqrt(new_second) + epsilon)).astype(BF16)
        back = nt(scaled, ql_ref[s]).astype(BF16)
        for j in range(PER):
            bt_ref[s * PER + j] = back[:, j * LANES : (j + 1) * LANES]

    send_all(exchange_z, NZ, bt_ref, b_ref, b_send, b_recv, src_at=True)
    b_ref[z] = bt_ref[z]
    stores.append(pltpu.make_async_copy(state_ref.at[0], moment_out, store_sem.at[0]))
    stores.append(pltpu.make_async_copy(state_ref.at[1], second_out, store_sem.at[1]))
    for store in stores:
        store.start()
    weight = (1.0 - stat_decay) * (factor * factor)
    for s in range(SLOTS):
        gt = gt_ref[s].reshape(BS, BS)
        rows = nt(pick_ref[...], gt).astype(BF16)
        state_ref[2, s] = stat_decay * state_ref[2, s] + weight * nn(rows, gt)
    stores.append(pltpu.make_async_copy(state_ref.at[2], left_out, store_sem.at[2]))
    stores[-1].start()

    b_all = all_of(b_ref, NZ, b_send, b_recv, "blk")
    b_all.wait_recv()
    stepped = nn(qr_ref[z // PER], b_ref[...].reshape(BS, LANES)).astype(BF16)
    ut_ref[...] = stepped.reshape(NZ, COLS, LANES)

    send_all(exchange_z, NZ, ut_ref, ur_ref, u_send, u_recv, src_at=True)
    ur_ref[z] = ut_ref[z]
    for s in range(SLOTS):
        gt = gt_ref[s].reshape(BS, BS)
        state_ref[3, s] = stat_decay * state_ref[3, s] + weight * nt(gt_ref[s, z], gt)
    stores.append(pltpu.make_async_copy(state_ref.at[3], right_out, store_sem.at[3]))
    stores[-1].start()

    u_all = all_of(ur_ref, NZ, u_send, u_recv, "blk")
    u_all.wait_recv()
    for s in range(SLOTS):
        for j in range(PER):
            u2_ref[pl.ds(s * COLS, COLS), pl.ds(j * LANES, LANES)] = ur_ref[s * PER + j]
    for g in range(2):
        rows = nt(spread_ref[...], u2_ref[:, pl.ds(g * wide, wide)]).astype(BF16)
        y_ref[pl.ds(g * (NF // 2), NF // 2)] = rows.reshape(NF // 2, PAD, LANES)

    send_all(exchange_f, NF, y_ref, w_ref, w_send, w_recv, src_at=True)
    w_ref[f, pl.ds(0, ROWS)] = y_ref[f, pl.ds(0, ROWS)]
    w_all = all_of(w_ref, NF, w_send, w_recv, "fsdp", ROWS)
    w_all.wait_recv()
    w_out[...] = w_ref[:, pl.ds(0, ROWS)]

    x_all.wait_send()
    plane_all.wait_send()
    all_all.wait_send()
    for hop in hops.values():
        hop.wait_send()
    b_all.wait_send()
    u_all.wait_send()
    w_all.wait_send()
    for store in stores:
        store.wait()


def body(grad, owner_slots, stat_left, stat_right, basis_left, basis_right, moment, second):
    blocks = grad.shape[0]
    chosen = (owner_slots[:, None] == jnp.arange(blocks, dtype=jnp.int32)[None, :]).astype(BF16)
    arranged = jnp.einsum("tb,brc->trc", chosen, grad, preferred_element_type=BF16)
    arranged = arranged.reshape(NF, SLOTS, ROWS, COLS).transpose(0, 2, 1, 3).reshape(NF, ROWS, LANES)

    state = jax.ShapeDtypeStruct((SLOTS, COLS, BS), F32)
    vmem = pl.BlockSpec(memory_space=pltpu.VMEM)
    any_ = pl.BlockSpec(memory_space=pl.ANY)
    dma = pltpu.SemaphoreType.DMA
    returned, new_left, new_right, new_moment, new_second, rms = pl.pallas_call(
        functools.partial(kernel, float(blocks * BS * BS)),
        out_shape=(
            jax.ShapeDtypeStruct((NF, ROWS, LANES), BF16),
            state,
            state,
            state,
            state,
            jax.ShapeDtypeStruct((8, LANES), F32),
        ),
        in_specs=[any_] * 7,
        out_specs=(vmem, any_, any_, any_, any_, vmem),
        scratch_shapes=[
            pltpu.VMEM((NF, ROWS, LANES), BF16),
            pltpu.VMEM((NF, PAD, LANES), BF16),
            pltpu.VMEM((SLOTS, NZ, COLS, BS), BF16),
            pltpu.VMEM((SLOTS, BS, BS), BF16),
            pltpu.VMEM((SLOTS, BS, BS), BF16),
            pltpu.VMEM((4, SLOTS, COLS, BS), F32),
            pltpu.VMEM((NF // 2 * PAD, BS // 2), BF16),
            pltpu.VMEM((COLS, BS), BF16),
            pltpu.VMEM((SLOTS, COLS, BS), BF16),
            pltpu.VMEM((8, LANES), F32),
            pltpu.VMEM((NF, 8, LANES), F32),
            pltpu.VMEM((8, LANES), F32),
            pltpu.VMEM((NZ, 8, LANES), F32),
            pltpu.VMEM((NZ, COLS, LANES), BF16),
            pltpu.VMEM((NZ, COLS, LANES), BF16),
            pltpu.VMEM((NZ, COLS, LANES), BF16),
            pltpu.VMEM((NZ, COLS, LANES), BF16),
            pltpu.VMEM((SLOTS * COLS, BS), BF16),
            pltpu.VMEM((NF, PAD, LANES), BF16),
            pltpu.VMEM((NF, PAD, LANES), BF16),
            dma((7,)),
            dma((4,)),
            dma((1,)),
            dma((1,)),
            dma((SLOTS, 2, PIECES, NZ // 2)),
            dma((SLOTS, 2, PIECES, NZ // 2)),
        ]
        + [dma((1,))] * 10,
        compiler_params=pltpu.CompilerParams(collective_id=0, has_side_effects=True),
    )(
        arranged,
        basis_left,
        basis_right,
        stat_left.swapaxes(1, 2),
        stat_right.swapaxes(1, 2),
        moment.swapaxes(1, 2),
        second.swapaxes(1, 2),
    )
    returned = returned.reshape(NF, ROWS, SLOTS, COLS).transpose(0, 2, 1, 3)
    returned = returned.reshape(blocks, ROWS, COLS)
    placed = jnp.einsum("tb,trc->brc", chosen, returned, preferred_element_type=BF16)
    return (
        placed,
        new_left.swapaxes(1, 2),
        new_right.swapaxes(1, 2),
        new_moment.swapaxes(1, 2),
        new_second.swapaxes(1, 2),
        rms[0, 0],
    )


def solution(mesh):
    rows = P(None, "fsdp", "blk")
    held = P("fsdp", None, "blk")
    whole = P("fsdp", None, None)
    return jax.shard_map(
        body,
        mesh=mesh,
        in_specs=(rows, P(), held, held, whole, whole, held, held),
        out_specs=(rows, held, held, held, held, P()),
        check_vma=False,
    )
```
